32 devices in a mesh: dp: 16 (over z, y, core), tp: 2 (over x).
Axes of the slice: x: 2, y: 2, z: 4, core: 2. Of those that a mesh axis runs over, the one named last changes fastest.
Arguments:
- hidden: bfloat16 [4096, 4096], P(('dp', 'tp')), may hold values from -6 to 6
- query_grad: bfloat16 [4096, 1024], P('dp', 'tp'), may hold values from -1.5 to 1.5
- key_grad: bfloat16 [4096, 256], P('dp', 'tp'), may hold values from -1.5 to 1.5
- value_grad: bfloat16 [4096, 256], P('dp', 'tp'), may hold values from -1.5 to 1.5
- w_query: bfloat16 [4096, 1024], P(None, 'tp'), may hold values from -0.09375 to 0.09375
- w_key: bfloat16 [4096, 256], P(None, 'tp'), may hold values from -0.09375 to 0.09375
- w_value: bfloat16 [4096, 256], P(None, 'tp'), may hold values from -0.09375 to 0.09375
Outputs:
- hidden_grad: bfloat16 [4096, 4096], P(('dp', 'tp'))
- grad_query: float32 [4096, 1024], P('dp', 'tp')
- grad_key: float32 [4096, 256], P('dp', 'tp')
- grad_value: float32 [4096, 256], P('dp', 'tp')
The draws below stay inside these ranges and needn't reach their ends.
All inputs are finite; a program needn't handle non-finite values.
Results may differ from the reference program's by a relative error of at most 0.014.
Values may be sent and summed in bfloat16 or wider, within the bound.
A program may use at most 256 MiB of HBM per device.

```python
import jax
import jax.numpy as jnp
from jax import lax

D = 4096
HEAD = 128
Q_DEV = 4
KV_HEADS = 2
Q_W = 1024
KV_W = 256
GROUP_TOK = 256
TOKENS = 4096
N_DP = 16


def raised(entries, key, source, target, blocks, factor):
    owner, partner = [(jnp.arange(entries.shape[position]) // (entries.shape[position] // blocks)).reshape([-1 if axis == position else 1 for axis in range(entries.ndim)]) for position in (source, target)]
    chosen = jax.random.permutation(key, blocks)[partner]
    strong = (owner == chosen) | (owner == (partner + blocks // 2) % blocks)
    return jnp.where(strong, factor * entries, entries)


def steps_of(stream_key, shape, shards, low, largest):
    gain, own = 1.0, jax.random.fold_in(stream_key, 6)
    for dim, blocks in shards:
        draws = jnp.exp(jax.random.uniform(jax.random.fold_in(own, dim), (blocks,), jnp.float32, low / len(shards), largest / len(shards)))
        gain = gain * jnp.repeat(draws, shape[dim] // blocks).reshape([-1 if axis == dim else 1 for axis in range(len(shape))])
    return gain


def gaussian(key, dims, scale, most, pieces=(), dtype=jnp.bfloat16):
    result = scale * jax.random.normal(key, dims, jnp.float32)
    if pieces:
        result = result * steps_of(key, dims, pieces, -0.22, 0.18)
    return jnp.clip(result, -most, most).astype(dtype)


def noise_with(stream_key, extent, scale, most, split, heavy, kind=jnp.bfloat16):
    array = scale * jax.random.normal(stream_key, extent, jnp.float32)
    if split:
        array = array * steps_of(stream_key, extent, split, -0.22, 0.18)
    return jnp.clip(raised(array, jax.random.fold_in(stream_key, 3), *heavy), -most, most).astype(kind)


def setup_inputs(seed: int = 0) -> dict:
    key_of = jax.random.split(jax.random.key(seed), 8)
    return {
        "hidden": noise_with(key_of[0], (TOKENS, D), 1.0, 6.0, ((0, 32),), (0, 1, 32, 2.75)),
        "query_grad": gaussian(key_of[1], (TOKENS, Q_W), 0.25, 1.5, ((0, 16), (1, 2))),
        "key_grad": gaussian(key_of[2], (TOKENS, KV_W), 0.25, 1.5, ((0, 16), (1, 2))),
        "value_grad": gaussian(key_of[3], (TOKENS, KV_W), 0.25, 1.5, ((0, 16), (1, 2))),
        "w_query": gaussian(key_of[4], (D, Q_W), D ** -0.5, 0.09375, ((1, 2),)),
        "w_key": gaussian(key_of[5], (D, KV_W), D ** -0.5, 0.09375, ((1, 2),)),
        "w_value": gaussian(key_of[6], (D, KV_W), D ** -0.5, 0.09375, ((1, 2),)),
    }


def contract_rows(left, right):
    return lax.dot_general(left, right, (((0,), (0,)), ((), ())), preferred_element_type=jnp.float32)


def rounded(value):
    return lax.optimization_barrier(value.astype(jnp.bfloat16)).astype(jnp.float32)


def reference(hidden, query_grad, key_grad, value_grad, w_query, w_key, w_value):
    hidden_groups = hidden.reshape(N_DP, GROUP_TOK, D)
    query_groups = query_grad.reshape(N_DP, GROUP_TOK, Q_W)
    key_groups = key_grad.reshape(N_DP, GROUP_TOK, KV_W)
    value_groups = value_grad.reshape(N_DP, GROUP_TOK, KV_W)
    weight_heads = jnp.concatenate((w_query.reshape(D, KV_HEADS, Q_DEV * HEAD), w_key.reshape(D, KV_HEADS, HEAD), w_value.reshape(D, KV_HEADS, HEAD)), axis=2).astype(jnp.float32)

    def one_group(totals, inputs):
        grad_wq, grad_wk, grad_wv = totals
        hid, qgr, kgr, vgr = inputs
        grad_heads = jnp.concatenate((qgr.reshape(GROUP_TOK, KV_HEADS, Q_DEV * HEAD), kgr.reshape(GROUP_TOK, KV_HEADS, HEAD), vgr.reshape(GROUP_TOK, KV_HEADS, HEAD)), axis=2).astype(jnp.float32)
        parts = jnp.einsum("thc,dhc->htd", grad_heads, weight_heads)
        hid_grad = jnp.sum(rounded(parts), axis=0).astype(jnp.bfloat16)
        grad_wq = grad_wq + rounded(contract_rows(hid, qgr))
        grad_wk = grad_wk + rounded(contract_rows(hid, kgr))
        grad_wv = grad_wv + rounded(contract_rows(hid, vgr))
        return (grad_wq, grad_wk, grad_wv), hid_grad

    zeros = (jnp.zeros((D, Q_W), jnp.float32), jnp.zeros((D, KV_W), jnp.float32), jnp.zeros((D, KV_W), jnp.float32))
    totals, outputs = lax.scan(one_group, zeros, (hidden_groups, query_groups, key_groups, value_groups))
    hidden_grad = outputs.reshape(TOKENS, D)
    return hidden_grad, totals[0], totals[1], totals[2]
```

```python
import functools

import jax
import jax.numpy as jnp
from jax import lax
from jax.experimental import pallas as pl
from jax.experimental.pallas import tpu as pltpu
from jax.sharding import PartitionSpec as P

MESH = pl.DeviceIdType.MESH


def contract_rows(left, right):
    return lax.dot_general(
        left, right, (((0,), (0,)), ((), ())), preferred_element_type=jnp.float32
    )


def contract_cols(left, right):
    return lax.dot_general(
        left, right, (((1,), (1,)), ((), ())), preferred_element_type=jnp.float32
    )


def local(hidden, query_grad, key_grad, value_grad, w_query, w_key, w_value):
    query_width = w_query.shape[1]
    head_width = w_key.shape[1]
    all_grads = jnp.concatenate((query_grad, key_grad, value_grad), axis=1)
    all_weights = jnp.concatenate((w_query, w_key, w_value), axis=1)
    total = contract_rows(lax.all_gather(hidden, "tp", axis=0, tiled=True), all_grads)
    summed = lax.psum_scatter(
        contract_cols(all_grads, all_weights).astype(jnp.bfloat16),
        "tp",
        scatter_dimension=0,
        tiled=True,
    )
    weight_grad = lax.psum_scatter(
        total.astype(jnp.bfloat16), "dp", scatter_dimension=0, tiled=True
    ).astype(jnp.float32)
    grad_query = weight_grad[:, :query_width]
    grad_key = weight_grad[:, query_width : query_width + head_width]
    grad_value = weight_grad[:, query_width + head_width :]
    return (summed, grad_query, grad_key, grad_value)


def kernel(
    n_z, pieces,
    hidden, query_grad, key_grad, value_grad, w_query, w_key, w_value,
    out_hidden, out_query, out_key, out_value,
    tokens, grads, weights, head_out, head_in, core_out, core_in,
    y_out, y_in, total, z_out, z_in, result, final,
    load_sem, tok_send, tok_recv, head_send, head_recv, core_send, core_recv,
    y_send, y_recv, z_send, z_recv, store_sem,
):
    dp = lax.axis_index("dp")
    tp = lax.axis_index("tp")
    core = lax.rem(dp, 2)
    y = lax.rem(dp // 2, 2)
    z = dp // 4
    half = hidden.shape[0]
    q_w = query_grad.shape[1]
    k_w = key_grad.shape[1]
    rows = final.shape[0]
    pair = 2 * rows
    width = hidden.shape[1] // pieces

    x_peer = (dp, 1 - tp)
    core_peer = (dp + 1 - 2 * core, tp)
    y_peer = (dp + 2 - 4 * y, tp)
    far_first = sorted(range(1, n_z), key=lambda o: -min(o, n_z - o)) + [0]
    z_of = [lax.rem(z + o, n_z) for o in far_first]

    def z_peer(k):
        return (z_of[k] * 4 + y * 2 + core, tp)

    mine = pl.ds(pl.multiple_of(tp * half, half), half)
    theirs = pl.ds(pl.multiple_of((1 - tp) * half, half), half)

    def load(index, source, target):
        copy = pltpu.make_async_copy(source, target, load_sem.at[index])
        copy.start()
        return copy

    loads = [
        load(0, query_grad, grads.at[:, pl.ds(0, q_w)]),
        load(1, key_grad, grads.at[:, pl.ds(q_w, k_w)]),
        load(2, value_grad, grads.at[:, pl.ds(q_w + k_w, k_w)]),
        load(3, hidden, tokens.at[mine, :]),
        load(4, w_query, weights.at[:, pl.ds(0, q_w)]),
        load(5, w_key, weights.at[:, pl.ds(q_w, k_w)]),
        load(6, w_value, weights.at[:, pl.ds(q_w + k_w, k_w)]),
    ]

    barrier = pltpu.get_barrier_semaphore()
    peers = [x_peer, core_peer, y_peer] + [z_peer(k) for k in range(n_z - 1)]
    for peer in peers:
        pl.semaphore_signal(barrier, inc=1, device_id=peer, device_id_type=MESH)
    pl.semaphore_wait(barrier, len(peers))

    def remote(source, target, send, recv, peer):
        return pltpu.make_async_remote_copy(
            src_ref=source, dst_ref=target, send_sem=send, recv_sem=recv,
            device_id=peer, device_id_type=MESH,
        )

    def pair_of(k):
        if k < n_z:
            return z_of[k] * 2 + (1 - y)
        return z_of[k - n_z] * 2 + y

    n_pairs = 2 * n_z
    tok_copies = []
    for k in range(n_pairs):
        columns = pl.ds(pl.multiple_of(pair_of(k) * pair, pair), pair)
        copy = remote(
            hidden.at[:, columns], tokens.at[mine, columns],
            tok_send.at[k], tok_recv.at[k], x_peer,
        )
        copy.start()
        tok_copies.append(copy)

    for copy in loads:
        copy.wait()

    def head_piece(j, carry):
        columns = pl.ds(pl.multiple_of(j * width, width), width)
        head_out[j] = contract_cols(
            grads[theirs, :], weights[columns, :]
        ).astype(head_out.dtype)
        return carry

    lax.fori_loop(0, pieces, head_piece, 0)

    head_copies = [
        remote(
            head_out.at[j], head_in.at[j], head_send.at[j], head_recv.at[j], x_peer
        )
        for j in range(pieces)
    ]
    core_copies = [
        remote(
            core_out.at[k], core_in.at[k], core_send.at[k], core_recv.at[k], core_peer
        )
        for k in range(n_pairs)
    ]
    y_copies = [
        remote(y_out.at[k], y_in.at[k], y_send.at[k], y_recv.at[k], y_peer)
        for k in range(n_z)
    ]
    z_copies = [
        remote(z_out.at[k], z_in.at[k], z_send.at[k], z_recv.at[k], z_peer(k))
        for k in range(n_z - 1)
    ]

    def block(k, which):
        start = pl.multiple_of(pair_of(k) * pair + which * rows, rows)
        return contract_rows(tokens[:, pl.ds(start, rows)], grads[...])

    def finish(k):
        core_copies[k].wait_recv()
        summed = block(k, core) + core_in[k].astype(jnp.float32)
        if k < n_z:
            y_out[k] = summed.astype(y_out.dtype)
            y_copies[k].start()
        else:
            total[k - n_z] = summed

    heads_started = 0
    for k in range(n_pairs):
        tok_copies[k].wait_recv()
        core_out[k] = block(k, 1 - core).astype(core_out.dtype)
        core_copies[k].start()
        if k >= 1:
            finish(k - 1)
        if k >= 1:
            stop = pieces * k // (n_pairs - 1)
            for j in range(heads_started, stop):
                head_copies[j].start()
            heads_started = stop
    finish(n_pairs - 1)

    def forward(k):
        y_copies[k].wait_recv()
        summed = total[k] + y_in[k].astype(jnp.float32)
        if k < n_z - 1:
            z_out[k] = summed.astype(z_out.dtype)
            z_copies[k].start()
        else:
            for s in range(n_z - 1):
                z_copies[s].wait_recv()
                summed = summed + z_in[s].astype(jnp.float32)
            final[...] = summed

    stores = []

    def add_heads(j):
        head_copies[j].wait_recv()
        columns = pl.ds(j * width, width)
        own = contract_cols(grads[mine, :], weights[columns, :])
        result[:, columns] = (own + head_in[j].astype(jnp.float32)).astype(result.dtype)
        copy = pltpu.make_async_copy(
            result.at[:, columns], out_hidden.at[:, columns], store_sem.at[j]
        )
        copy.start()
        stores.append(copy)

    ready = 0
    for k in range(n_z):
        forward(k)
        if k < n_z - 1:
            stop = (pieces - 2) * k // max(n_z - 2, 1)
            for j in range(ready, stop):
                add_heads(j)
            ready = max(stop, ready)
    for index, (target, start, size) in enumerate(
        ((out_query, 0, q_w), (out_key, q_w, k_w), (out_value, q_w + k_w, k_w))
    ):
        copy = pltpu.make_async_copy(
            final.at[:, pl.ds(start, size)], target, store_sem.at[pieces + index]
        )
        copy.start()
        stores.append(copy)
    for j in range(ready, pieces):
        add_heads(j)
    for copy in tok_copies + head_copies + core_copies + y_copies + z_copies:
        copy.wait_send()
    for copy in stores:
        copy.wait()


def fused(n_dp, hidden, query_grad, key_grad, value_grad, w_query, w_key, w_value):
    half, depth = hidden.shape
    group = query_grad.shape[0]
    q_w, k_w = w_query.shape[1], w_key.shape[1]
    wide = q_w + 2 * k_w
    rows = depth // n_dp
    n_z = n_dp // 4
    n_pairs = 2 * n_z
    pieces = n_pairs
    width = depth // pieces
    bf16, f32 = jnp.bfloat16, jnp.float32
    dma = pltpu.SemaphoreType.DMA
    return pl.pallas_call(
        functools.partial(kernel, n_z, pieces),
        out_shape=(
            jax.ShapeDtypeStruct((half, depth), bf16),
            jax.ShapeDtypeStruct((rows, q_w), f32),
            jax.ShapeDtypeStruct((rows, k_w), f32),
            jax.ShapeDtypeStruct((rows, k_w), f32),
        ),
        in_specs=[pl.BlockSpec(memory_space=pl.ANY)] * 7,
        out_specs=(pl.BlockSpec(memory_space=pl.ANY),) * 4,
        scratch_shapes=[
            pltpu.VMEM((group, depth), bf16),
            pltpu.VMEM((group, wide), bf16),
            pltpu.VMEM((depth, wide), bf16),
            pltpu.VMEM((pieces, half, width), bf16),
            pltpu.VMEM((pieces, half, width), bf16),
            pltpu.VMEM((n_pairs, rows, wide), bf16),
            pltpu.VMEM((n_pairs, rows, wide), bf16),
            pltpu.VMEM((n_z, rows, wide), bf16),
            pltpu.VMEM((n_z, rows, wide), bf16),
            pltpu.VMEM((n_z, rows, wide), f32),
            pltpu.VMEM((n_z - 1, rows, wide), bf16),
            pltpu.VMEM((n_z - 1, rows, wide), bf16),
            pltpu.VMEM((half, depth), bf16),
            pltpu.VMEM((rows, wide), f32),
            dma((7,)),
            dma((n_pairs,)), dma((n_pairs,)),
            dma((pieces,)), dma((pieces,)),
            dma((n_pairs,)), dma((n_pairs,)),
            dma((n_z,)), dma((n_z,)),
            dma((n_z - 1,)), dma((n_z - 1,)),
            dma((pieces + 3,)),
        ],
        compiler_params=pltpu.CompilerParams(
            collective_id=0, has_side_effects=True, vmem_limit_bytes=56 * 1024 * 1024
        ),
    )(hidden, query_grad, key_grad, value_grad, w_query, w_key, w_value)


def solution(mesh):
    placed = (
        P(("dp", "tp"), None),
        P("dp", "tp"),
        P("dp", "tp"),
        P("dp", "tp"),
        P(None, "tp"),
        P(None, "tp"),
        P(None, "tp"),
    )
    n_dp, n_tp = mesh.shape["dp"], mesh.shape["tp"]
    body = local
    if n_tp == 2 and n_dp % 4 == 0 and n_dp > 4:
        body = functools.partial(fused, n_dp)
    return jax.shard_map(
        body,
        mesh=mesh,
        in_specs=placed,
        out_specs=(P(("dp", "tp"), None), P("dp", "tp"), P("dp", "tp"), P("dp", "tp")),
        check_vma=False,
    )
```

```python
import functools

import jax
import jax.numpy as jnp
from jax import lax
from jax.experimental import pallas as pl
from jax.experimental.pallas import tpu as pltpu
from jax.sharding import PartitionSpec as P

MESH = pl.DeviceIdType.MESH


def contract_rows(left, right):
    return lax.dot_general(
        left, right, (((0,), (0,)), ((), ())), preferred_element_type=jnp.float32
    )


def contract_cols(left, right):
    return lax.dot_general(
        left, right, (((1,), (1,)), ((), ())), preferred_element_type=jnp.float32
    )


def local(hidden, query_grad, key_grad, value_grad, w_query, w_key, w_value):
    query_width = w_query.shape[1]
    head_width = w_key.shape[1]
    all_grads = jnp.concatenate((query_grad, key_grad, value_grad), axis=1)
    all_weights = jnp.concatenate((w_query, w_key, w_value), axis=1)
    total = contract_rows(lax.all_gather(hidden, "tp", axis=0, tiled=True), all_grads)
    summed = lax.psum_scatter(
        contract_cols(all_grads, all_weights).astype(jnp.bfloat16),
        "tp",
        scatter_dimension=0,
        tiled=True,
    )
    weight_grad = lax.psum_scatter(
        total.astype(jnp.bfloat16), "dp", scatter_dimension=0, tiled=True
    ).astype(jnp.float32)
    grad_query = weight_grad[:, :query_width]
    grad_key = weight_grad[:, query_width : query_width + head_width]
    grad_value = weight_grad[:, query_width + head_width :]
    return (summed, grad_query, grad_key, grad_value)


def kernel(
    n_z, pieces,
    hidden, query_grad, key_grad, value_grad, w_query, w_key, w_value,
    result, final,
    tokens, grads, weights, head_out, head_in, core_out, core_in,
    y_out, y_in, total, z_out, z_in,
    load_sem, tok_send, tok_recv, head_send, head_recv, core_send, core_recv,
    y_send, y_recv, z_send, z_recv,
):
    dp = lax.axis_index("dp")
    tp = lax.axis_index("tp")
    core = lax.rem(dp, 2)
    y = lax.rem(dp // 2, 2)
    z = dp // 4
    half = hidden.shape[0]
    q_w = query_grad.shape[1]
    k_w = key_grad.shape[1]
    rows = final.shape[0]
    pair = 2 * rows
    width = hidden.shape[1] // pieces

    x_peer = (dp, 1 - tp)
    core_peer = (dp + 1 - 2 * core, tp)
    y_peer = (dp + 2 - 4 * y, tp)
    far_first = sorted(range(1, n_z), key=lambda o: -min(o, n_z - o)) + [0]
    z_of = [lax.rem(z + o, n_z) for o in far_first]

    def z_peer(k):
        return (z_of[k] * 4 + y * 2 + core, tp)

    mine = pl.ds(pl.multiple_of(tp * half, half), half)
    theirs = pl.ds(pl.multiple_of((1 - tp) * half, half), half)

    def load(index, source, target):
        copy = pltpu.make_async_copy(source, target, load_sem.at[index])
        copy.start()
        return copy

    loads = [
        load(0, query_grad, grads.at[:, pl.ds(0, q_w)]),
        load(1, key_grad, grads.at[:, pl.ds(q_w, k_w)]),
        load(2, value_grad, grads.at[:, pl.ds(q_w + k_w, k_w)]),
        load(3, hidden, tokens.at[mine, :]),
        load(4, w_query, weights.at[:, pl.ds(0, q_w)]),
        load(5, w_key, weights.at[:, pl.ds(q_w, k_w)]),
        load(6, w_value, weights.at[:, pl.ds(q_w + k_w, k_w)]),
    ]

    barrier = pltpu.get_barrier_semaphore()
    peers = [x_peer, core_peer, y_peer] + [z_peer(k) for k in range(n_z - 1)]
    for peer in peers:
        pl.semaphore_signal(barrier, inc=1, device_id=peer, device_id_type=MESH)
    pl.semaphore_wait(barrier, len(peers))

    def remote(source, target, send, recv, peer):
        return pltpu.make_async_remote_copy(
            src_ref=source, dst_ref=target, send_sem=send, recv_sem=recv,
            device_id=peer, device_id_type=MESH,
        )

    def pair_of(k):
        if k < n_z:
            return z_of[k] * 2 + (1 - y)
        return z_of[k - n_z] * 2 + y

    n_pairs = 2 * n_z
    tok_copies = []
    for k in range(n_pairs):
        columns = pl.ds(pl.multiple_of(pair_of(k) * pair, pair), pair)
        copy = remote(
            hidden.at[:, columns], tokens.at[mine, columns],
            tok_send.at[k], tok_recv.at[k], x_peer,
        )
        copy.start()
        tok_copies.append(copy)

    for copy in loads[:4]:
        copy.wait()

    head_copies = [
        remote(
            head_out.at[j], head_in.at[j], head_send.at[j], head_recv.at[j], x_peer
        )
        for j in range(pieces)
    ]
    core_copies = [
        remote(
            core_out.at[k], core_in.at[k], core_send.at[k], core_recv.at[k], core_peer
        )
        for k in range(n_pairs)
    ]
    y_copies = [
        [
            remote(
                y_out.at[k, h], y_in.at[k, h],
                y_send.at[k, h], y_recv.at[k, h], y_peer,
            )
            for h in range(2)
        ]
        for k in range(n_z)
    ]
    z_copies = [
        [
            remote(
                z_out.at[k, h], z_in.at[k, h],
                z_send.at[k, h], z_recv.at[k, h], z_peer(k),
            )
            for h in range(2)
        ]
        for k in range(n_z - 1)
    ]
    part = rows // 2

    def block(k, which, first, size):
        start = pl.multiple_of(pair_of(k) * pair + which * rows + first, part)
        return contract_rows(tokens[:, pl.ds(start, size)], grads[...])

    def finish(k):
        for h in range(2):
            own = block(k, core, h * part, part)
            if h == 0:
                core_copies[k].wait_recv()
            span = pl.ds(h * part, part)
            summed = own + core_in[k, span].astype(jnp.float32)
            if k < n_z:
                y_out[k, h] = summed.astype(y_out.dtype)
                y_copies[k][h].start()
            else:
                total[k - n_z, h] = summed

    def head_piece(j):
        columns = pl.ds(j * width, width)
        head_out[j] = contract_cols(
            grads[theirs, :], weights[columns, :]
        ).astype(head_out.dtype)
        head_copies[j].start()

    def forward(k, h):
        y_copies[k][h].wait_recv()
        summed = total[k, h] + y_in[k, h].astype(jnp.float32)
        if k < n_z - 1:
            z_out[k, h] = summed.astype(z_out.dtype)
            z_copies[k][h].start()
        else:
            total[k, h] = summed

    for k in range(n_pairs):
        tok_copies[k].wait_recv()
        core_out[k] = block(k, 1 - core, 0, rows).astype(core_out.dtype)
        core_copies[k].start()
        finish(k)
        if k == 0:
            for copy in loads[4:]:
                copy.wait()
        head_piece(k)
        if k == n_z:
            forward(0, 0)
            forward(0, 1)
    assert pieces == n_pairs

    def add_heads(j):
        head_copies[j].wait_recv()
        columns = pl.ds(j * width, width)
        own = contract_cols(grads[mine, :], weights[columns, :])
        result[:, columns] = (own + head_in[j].astype(jnp.float32)).astype(result.dtype)

    ready = 0
    for k in range(1, n_z):
        stop = (pieces - 1) * k // n_z
        for h in range(2):
            forward(k, h)
        for j in range(ready, stop):
            add_heads(j)
        ready = stop
    for h in range(2):
        span = pl.ds(h * part, part)
        summed = total[n_z - 1, h]
        for s in range(n_z - 1):
            z_copies[s][h].wait_recv()
            summed = summed + z_in[s, h].astype(jnp.float32)
        final[span, :] = summed
    for j in range(ready, pieces):
        add_heads(j)
    flat = [copy for pair in y_copies + z_copies for copy in pair]
    for copy in tok_copies + head_copies + core_copies + flat:
        copy.wait_send()


def place(result, final, out_hidden, out_query, out_key, out_value, sem):
    q_w, k_w = out_query.shape[1], out_key.shape[1]
    copies = [
        pltpu.make_async_copy(result, out_hidden, sem.at[0]),
        pltpu.make_async_copy(final.at[:, pl.ds(0, q_w)], out_query, sem.at[1]),
        pltpu.make_async_copy(final.at[:, pl.ds(q_w, k_w)], out_key, sem.at[2]),
        pltpu.make_async_copy(
            final.at[:, pl.ds(q_w + k_w, k_w)], out_value, sem.at[3]
        ),
    ]
    for copy in copies:
        copy.start()
    for copy in copies:
        copy.wait()


def fused(n_dp, hidden, query_grad, key_grad, value_grad, w_query, w_key, w_value):
    half, depth = hidden.shape
    group = query_grad.shape[0]
    q_w, k_w = w_query.shape[1], w_key.shape[1]
    wide = q_w + 2 * k_w
    rows = depth // n_dp
    n_z = n_dp // 4
    n_pairs = 2 * n_z
    pieces = n_pairs
    width = depth // pieces
    bf16, f32 = jnp.bfloat16, jnp.float32
    dma = pltpu.SemaphoreType.DMA
    held = pl.pallas_call(
        functools.partial(kernel, n_z, pieces),
        out_shape=(pltpu.VMEM((half, depth), bf16), pltpu.VMEM((rows, wide), f32)),
        in_specs=[pl.BlockSpec(memory_space=pl.ANY)] * 7,
        out_specs=(pl.BlockSpec(memory_space=pltpu.VMEM),) * 2,
        scratch_shapes=[
            pltpu.VMEM((group, depth), bf16),
            pltpu.VMEM((group, wide), bf16),
            pltpu.VMEM((depth, wide), bf16),
            pltpu.VMEM((pieces, half, width), bf16),
            pltpu.VMEM((pieces, half, width), bf16),
            pltpu.VMEM((n_pairs, rows, wide), bf16),
            pltpu.VMEM((n_pairs, rows, wide), bf16),
            pltpu.VMEM((n_z, 2, rows // 2, wide), bf16),
            pltpu.VMEM((n_z, 2, rows // 2, wide), bf16),
            pltpu.VMEM((n_z, 2, rows // 2, wide), f32),
            pltpu.VMEM((n_z - 1, 2, rows // 2, wide), bf16),
            pltpu.VMEM((n_z - 1, 2, rows // 2, wide), bf16),
            dma((7,)),
            dma((n_pairs,)), dma((n_pairs,)),
            dma((pieces,)), dma((pieces,)),
            dma((n_pairs,)), dma((n_pairs,)),
            dma((n_z, 2)), dma((n_z, 2)),
            dma((n_z - 1, 2)), dma((n_z - 1, 2)),
        ],
        compiler_params=pltpu.CompilerParams(
            collective_id=0, has_side_effects=True, vmem_limit_bytes=56 * 1024 * 1024
        ),
    )(hidden, query_grad, key_grad, value_grad, w_query, w_key, w_value)
    return pl.pallas_call(
        place,
        out_shape=(
            jax.ShapeDtypeStruct((half, depth), bf16),
            jax.ShapeDtypeStruct((rows, q_w), f32),
            jax.ShapeDtypeStruct((rows, k_w), f32),
            jax.ShapeDtypeStruct((rows, k_w), f32),
        ),
        in_specs=[pl.BlockSpec(memory_space=pltpu.VMEM)] * 2,
        out_specs=(pl.BlockSpec(memory_space=pl.ANY),) * 4,
        scratch_shapes=[dma((4,))],
    )(*[pltpu.with_memory_space_constraint(a, pltpu.VMEM) for a in held])


def solution(mesh):
    placed = (
        P(("dp", "tp"), None),
        P("dp", "tp"),
        P("dp", "tp"),
        P("dp", "tp"),
        P(None, "tp"),
        P(None, "tp"),
        P(None, "tp"),
    )
    n_dp, n_tp = mesh.shape["dp"], mesh.shape["tp"]
    body = local
    if n_tp == 2 and n_dp % 4 == 0 and n_dp > 4:
        body = functools.partial(fused, n_dp)
    return jax.shard_map(
        body,
        mesh=mesh,
        in_specs=placed,
        out_specs=(P(("dp", "tp"), None), P("dp", "tp"), P("dp", "tp"), P("dp", "tp")),
        check_vma=False,
    )
```

```python
import functools

import jax
import jax.numpy as jnp
from jax import lax
from jax.experimental import pallas as pl
from jax.experimental.pallas import tpu as pltpu
from jax.sharding import PartitionSpec as P

MESH = pl.DeviceIdType.MESH


def contract_rows(left, right):
    return lax.dot_general(
        left, right, (((0,), (0,)), ((), ())), preferred_element_type=jnp.float32
    )


def contract_cols(left, right):
    return lax.dot_general(
        left, right, (((1,), (1,)), ((), ())), preferred_element_type=jnp.float32
    )


def local(hidden, query_grad, key_grad, value_grad, w_query, w_key, w_value):
    query_width = w_query.shape[1]
    head_width = w_key.shape[1]
    all_grads = jnp.concatenate((query_grad, key_grad, value_grad), axis=1)
    all_weights = jnp.concatenate((w_query, w_key, w_value), axis=1)
    total = contract_rows(lax.all_gather(hidden, "tp", axis=0, tiled=True), all_grads)
    summed = lax.psum_scatter(
        contract_cols(all_grads, all_weights).astype(jnp.bfloat16),
        "tp",
        scatter_dimension=0,
        tiled=True,
    )
    weight_grad = lax.psum_scatter(
        total.astype(jnp.bfloat16), "dp", scatter_dimension=0, tiled=True
    ).astype(jnp.float32)
    grad_query = weight_grad[:, :query_width]
    grad_key = weight_grad[:, query_width : query_width + head_width]
    grad_value = weight_grad[:, query_width + head_width :]
    return (summed, grad_query, grad_key, grad_value)


def kernel(
    n_z, pieces,
    hidden, query_grad, key_grad, value_grad, w_query, w_key, w_value,
    result, final,
    tokens, grads, weights, head_out, head_in, core_out, core_in,
    y_out, y_in, total, z_out, z_in,
    load_sem, tok_send, tok_recv, head_send, head_recv, core_send, core_recv,
    y_send, y_recv, z_send, z_recv,
):
    dp = lax.axis_index("dp")
    tp = lax.axis_index("tp")
    core = lax.rem(dp, 2)
    y = lax.rem(dp // 2, 2)
    z = dp // 4
    half = hidden.shape[0]
    q_w = query_grad.shape[1]
    k_w = key_grad.shape[1]
    rows = final.shape[0]
    pair = 2 * rows
    width = hidden.shape[1] // pieces

    x_peer = (dp, 1 - tp)
    core_peer = (dp + 1 - 2 * core, tp)
    y_peer = (dp + 2 - 4 * y, tp)
    far_first = sorted(range(1, n_z), key=lambda o: -min(o, n_z - o)) + [0]
    z_of = [lax.rem(z + o, n_z) for o in far_first]

    def z_peer(k):
        return (z_of[k] * 4 + y * 2 + core, tp)

    mine = pl.ds(pl.multiple_of(tp * half, half), half)
    theirs = pl.ds(pl.multiple_of((1 - tp) * half, half), half)

    def load(index, source, target):
        copy = pltpu.make_async_copy(source, target, load_sem.at[index])
        copy.start()
        return copy

    loads = [
        load(0, query_grad, grads.at[:, pl.ds(0, q_w)]),
        load(1, key_grad, grads.at[:, pl.ds(q_w, k_w)]),
        load(2, value_grad, grads.at[:, pl.ds(q_w + k_w, k_w)]),
        load(3, hidden, tokens.at[mine, :]),
        load(4, w_query, weights.at[:, pl.ds(0, q_w)]),
        load(5, w_key, weights.at[:, pl.ds(q_w, k_w)]),
        load(6, w_value, weights.at[:, pl.ds(q_w + k_w, k_w)]),
    ]

    barrier = pltpu.get_barrier_semaphore()
    peers = [x_peer, core_peer, y_peer] + [z_peer(k) for k in range(n_z - 1)]
    for peer in peers:
        pl.semaphore_signal(barrier, inc=1, device_id=peer, device_id_type=MESH)
    pl.semaphore_wait(barrier, len(peers))

    def remote(source, target, send, recv, peer):
        return pltpu.make_async_remote_copy(
            src_ref=source, dst_ref=target, send_sem=send, recv_sem=recv,
            device_id=peer, device_id_type=MESH,
        )

    def pair_of(k):
        return z_of[k // 2] * 2 + (1 - y if k % 2 == 0 else y)

    n_pairs = 2 * n_z
    tok_copies = []
    for k in range(n_pairs):
        columns = pl.ds(pl.multiple_of(pair_of(k) * pair, pair), pair)
        copy = remote(
            hidden.at[:, columns], tokens.at[mine, columns],
            tok_send.at[k], tok_recv.at[k], x_peer,
        )
        copy.start()
        tok_copies.append(copy)

    for copy in loads[:4]:
        copy.wait()

    head_copies = [
        remote(
            head_out.at[j], head_in.at[j], head_send.at[j], head_recv.at[j], x_peer
        )
        for j in range(pieces)
    ]
    core_copies = [
        remote(
            core_out.at[k], core_in.at[k], core_send.at[k], core_recv.at[k], core_peer
        )
        for k in range(n_pairs)
    ]
    y_copies = [
        [
            remote(
                y_out.at[k, h], y_in.at[k, h],
                y_send.at[k, h], y_recv.at[k, h], y_peer,
            )
            for h in range(2)
        ]
        for k in range(n_z)
    ]
    z_copies = [
        [
            remote(
                z_out.at[k, h], z_in.at[k, h],
                z_send.at[k, h], z_recv.at[k, h], z_peer(k),
            )
            for h in range(2)
        ]
        for k in range(n_z - 1)
    ]
    part = rows // 2

    def block(k, which, first, size):
        start = pl.multiple_of(pair_of(k) * pair + which * rows + first, part)
        return contract_rows(tokens[:, pl.ds(start, size)], grads[...])

    def finish(k):
        for h in range(2):
            own = block(k, core, h * part, part)
            if h == 0:
                core_copies[k].wait_recv()
            span = pl.ds(h * part, part)
            summed = own + core_in[k, span].astype(jnp.float32)
            if k % 2 == 0:
                y_out[k // 2, h] = summed.astype(y_out.dtype)
                y_copies[k // 2][h].start()
            else:
                total[k // 2, h] = summed

    def head_piece(j):
        columns = pl.ds(j * width, width)
        head_out[j] = contract_cols(
            grads[theirs, :], weights[columns, :]
        ).astype(head_out.dtype)
        head_copies[j].start()

    def forward(k, h):
        y_copies[k][h].wait_recv()
        summed = total[k, h] + y_in[k, h].astype(jnp.float32)
        if k < n_z - 1:
            z_out[k, h] = summed.astype(z_out.dtype)
            z_copies[k][h].start()
        else:
            total[k, h] = summed

    sent = 0
    for k in range(n_pairs):
        tok_copies[k].wait_recv()
        core_out[k] = block(k, 1 - core, 0, rows).astype(core_out.dtype)
        core_copies[k].start()
        finish(k)
        if k == 0:
            for copy in loads[4:]:
                copy.wait()
        head_piece(k)
        if k >= 2 and k % 3 != 0:
            forward(sent // 2, sent % 2)
            sent += 1
    assert pieces == n_pairs

    def add_heads(j):
        head_copies[j].wait_recv()
        columns = pl.ds(j * width, width)
        own = contract_cols(grads[mine, :], weights[columns, :])
        result[:, columns] = (own + head_in[j].astype(jnp.float32)).astype(result.dtype)

    ready = 0
    for step in range(sent, 2 * n_z):
        forward(step // 2, step % 2)
        stop = (pieces - 1) * (step + 1 - sent) // (2 * n_z - sent)
        for j in range(ready, stop):
            add_heads(j)
        ready = stop
    for h in range(2):
        span = pl.ds(h * part, part)
        summed = total[n_z - 1, h]
        for s in range(n_z - 1):
            z_copies[s][h].wait_recv()
            summed = summed + z_in[s, h].astype(jnp.float32)
        final[span, :] = summed
    for j in range(ready, pieces):
        add_heads(j)
    flat = [copy for pair in y_copies + z_copies for copy in pair]
    for copy in tok_copies + head_copies + core_copies + flat:
        copy.wait_send()


def place(result, final, out_hidden, out_query, out_key, out_value, sem):
    q_w, k_w = out_query.shape[1], out_key.shape[1]
    copies = [
        pltpu.make_async_copy(result, out_hidden, sem.at[0]),
        pltpu.make_async_copy(final.at[:, pl.ds(0, q_w)], out_query, sem.at[1]),
        pltpu.make_async_copy(final.at[:, pl.ds(q_w, k_w)], out_key, sem.at[2]),
        pltpu.make_async_copy(
            final.at[:, pl.ds(q_w + k_w, k_w)], out_value, sem.at[3]
        ),
    ]
    for copy in copies:
        copy.start()
    for copy in copies:
        copy.wait()


def fused(n_dp, hidden, query_grad, key_grad, value_grad, w_query, w_key, w_value):
    half, depth = hidden.shape
    group = query_grad.shape[0]
    q_w, k_w = w_query.shape[1], w_key.shape[1]
    wide = q_w + 2 * k_w
    rows = depth // n_dp
    n_z = n_dp // 4
    n_pairs = 2 * n_z
    pieces = n_pairs
    width = depth // pieces
    bf16, f32 = jnp.bfloat16, jnp.float32
    dma = pltpu.SemaphoreType.DMA
    held = pl.pallas_call(
        functools.partial(kernel, n_z, pieces),
        out_shape=(pltpu.VMEM((half, depth), bf16), pltpu.VMEM((rows, wide), f32)),
        in_specs=[pl.BlockSpec(memory_space=pl.ANY)] * 7,
        out_specs=(pl.BlockSpec(memory_space=pltpu.VMEM),) * 2,
        scratch_shapes=[
            pltpu.VMEM((group, depth), bf16),
            pltpu.VMEM((group, wide), bf16),
            pltpu.VMEM((depth, wide), bf16),
            pltpu.VMEM((pieces, half, width), bf16),
            pltpu.VMEM((pieces, half, width), bf16),
            pltpu.VMEM((n_pairs, rows, wide), bf16),
            pltpu.VMEM((n_pairs, rows, wide), bf16),
            pltpu.VMEM((n_z, 2, rows // 2, wide), bf16),
            pltpu.VMEM((n_z, 2, rows // 2, wide), bf16),
            pltpu.VMEM((n_z, 2, rows // 2, wide), f32),
            pltpu.VMEM((n_z - 1, 2, rows // 2, wide), bf16),
            pltpu.VMEM((n_z - 1, 2, rows // 2, wide), bf16),
            dma((7,)),
            dma((n_pairs,)), dma((n_pairs,)),
            dma((pieces,)), dma((pieces,)),
            dma((n_pairs,)), dma((n_pairs,)),
            dma((n_z, 2)), dma((n_z, 2)),
            dma((n_z - 1, 2)), dma((n_z - 1, 2)),
        ],
        compiler_params=pltpu.CompilerParams(
            collective_id=0, has_side_effects=True, vmem_limit_bytes=56 * 1024 * 1024
        ),
    )(hidden, query_grad, key_grad, value_grad, w_query, w_key, w_value)
    return pl.pallas_call(
        place,
        out_shape=(
            jax.ShapeDtypeStruct((half, depth), bf16),
            jax.ShapeDtypeStruct((rows, q_w), f32),
            jax.ShapeDtypeStruct((rows, k_w), f32),
            jax.ShapeDtypeStruct((rows, k_w), f32),
        ),
        in_specs=[pl.BlockSpec(memory_space=pltpu.VMEM)] * 2,
        out_specs=(pl.BlockSpec(memory_space=pl.ANY),) * 4,
        scratch_shapes=[dma((4,))],
    )(*[pltpu.with_memory_space_constraint(a, pltpu.VMEM) for a in held])


def solution(mesh):
    placed = (
        P(("dp", "tp"), None),
        P("dp", "tp"),
        P("dp", "tp"),
        P("dp", "tp"),
        P(None, "tp"),
        P(None, "tp"),
        P(None, "tp"),
    )
    n_dp, n_tp = mesh.shape["dp"], mesh.shape["tp"]
    body = local
    if n_tp == 2 and n_dp % 4 == 0 and n_dp > 4:
        body = functools.partial(fused, n_dp)
    return jax.shard_map(
        body,
        mesh=mesh,
        in_specs=placed,
        out_specs=(P(("dp", "tp"), None), P("dp", "tp"), P("dp", "tp"), P("dp", "tp")),
        check_vma=False,
    )
```
